128 devices in a mesh: dp: 2 (over z_hi), seq: 16 (over y, x), tensor: 4 (over z_lo, core).
Axes of the slice: x: 4, y: 4, z: 4 (z_hi: 2, z_lo: 2; z = z_hi * 2 + z_lo), core: 2. Of those that a mesh axis runs over, the one named last changes fastest.
Arguments:
- incoming_activations: bfloat16 [2, 8192, 4096], P('dp', 'seq', 'tensor'), may hold values from -6 to 6
- objective_cotangents: bfloat16 [2, 8192, 4096], P('dp', 'seq', 'tensor'), may hold values from -400 to 400
- fixed_gating_kernel: bfloat16 [4096, 7168], P('seq', 'tensor'), may hold values from -0.09375 to 0.09375
- fixed_raising_kernel: bfloat16 [4096, 7168], P('seq', 'tensor'), may hold values from -1 to 1
- correction_narrower: bfloat16 [16, 7168], P(None, 'tensor'), may hold values from -0.0625 to 0.0625
- correction_widener: bfloat16 [16, 4096], P(None, 'tensor'), may hold values from -1.5 to 1.5
- cutoff_limits: float32 [2], replicated, may hold values from 100 to 400
Outputs:
- grad_a: float32 [16, 7168], P(None, 'tensor')
- grad_b: float32 [16, 4096], P(None, 'tensor')
The draws below stay inside these ranges and needn't reach their ends.
All inputs are finite; a program needn't handle non-finite values.
Results may differ from the reference program's by a relative error of at most 0.0041.
Values may be sent and summed in bfloat16 or wider, within the bound.
No kernel may reach another device: no remote copies, remote signals or barrier semaphores. Data moves between devices by JAX's collectives and lax.ppermute only.
A program may use at most 128 MiB of HBM per device.

```python
import math
import jax
import jax.numpy as jnp
from jax import lax

EMBEDDING_SPAN = 4096
INNER_NEURONS = 7168
CORRECTION_ORDER = 16
LENGTH = 8192
DOCS = 2


def draw_objective_cotangents(key, part):
    first = jax.random.fold_in(key, 11)
    second = jax.random.fold_in(key, 12)
    place = jnp.arange(LENGTH, dtype=jnp.float32) / LENGTH
    base = jax.random.truncated_normal(first, -4.0, 4.0, (DOCS, LENGTH, EMBEDDING_SPAN), jnp.float32)
    row = jnp.exp(jax.random.uniform(second, (DOCS, LENGTH, 1), jnp.float32, 0.0, 2.3))
    rise = jnp.exp(place * 1.0986)[None, :, None]
    values = base * row * rise
    return values.astype(jnp.bfloat16)


def draw_fixed_raising_kernel(key, part):
    first = jax.random.fold_in(key, 21)
    scale = EMBEDDING_SPAN ** (-0.5)
    values = jax.random.truncated_normal(first, -4.0, 4.0, (EMBEDDING_SPAN, INNER_NEURONS), jnp.float32) * scale
    return values.astype(jnp.bfloat16)


def block_levels(rng, shape, split, least, largest):
    level, own = 1.0, jax.random.fold_in(rng, 6)
    for axis_at, parts in split:
        heights = jnp.exp(jax.random.uniform(jax.random.fold_in(own, axis_at), (parts,), jnp.float32, least / len(split), largest / len(split)))
        level = level * jnp.repeat(heights, shape[axis_at] // parts).reshape([-1 if axis == axis_at else 1 for axis in range(len(shape))])
    return level


def bell_draw(stream_key, shape, deviation, most, pieces=(), kind=jnp.bfloat16):
    loudness = block_levels(stream_key, shape, pieces, -0.22, 0.18) if pieces else 1.0
    values = jax.random.normal(stream_key, shape, jnp.float32) * deviation * loudness
    return jnp.minimum(jnp.maximum(values, -most), most).astype(kind)


def setup_inputs(seed: int = 0) -> dict:
    arg_keys = jax.random.split(jax.random.key(seed), 8)
    incoming_activations = bell_draw(arg_keys[0], (DOCS, LENGTH, EMBEDDING_SPAN), 1.0, 6.0, ((0, 2), (1, 16), (2, 4)))
    objective_cotangents = draw_objective_cotangents(jax.random.fold_in(arg_keys[7], 71), 0)
    fixed_gating_kernel = bell_draw(arg_keys[2], (EMBEDDING_SPAN, INNER_NEURONS), EMBEDDING_SPAN ** -0.5, 0.09375, ((0, 16), (1, 4)))
    fixed_raising_kernel = draw_fixed_raising_kernel(jax.random.fold_in(arg_keys[7], 71), 0)
    correction_narrower = bell_draw(arg_keys[4], (CORRECTION_ORDER, INNER_NEURONS), INNER_NEURONS ** -0.5, 0.0625, ((1, 4),))
    correction_widener = bell_draw(arg_keys[5], (CORRECTION_ORDER, EMBEDDING_SPAN), CORRECTION_ORDER ** -0.5, 1.5, ((1, 4),))
    cutoff_limits = jnp.clip(jnp.exp(jax.random.uniform(arg_keys[6], (2,), jnp.float32, math.log(100.0), math.log(400.0))), 100.0, 400.0)
    return {"incoming_activations": incoming_activations, "objective_cotangents": objective_cotangents, "fixed_gating_kernel": fixed_gating_kernel, "fixed_raising_kernel": fixed_raising_kernel, "correction_narrower": correction_narrower, "correction_widener": correction_widener, "cutoff_limits": cutoff_limits}


def example_contributions(example_matching, fixed_gating_kernel, fixed_raising_kernel, correction_narrower, correction_widener):
    incoming_activations, objective_cotangents = example_matching
    gate = jnp.dot(incoming_activations, fixed_gating_kernel, preferred_element_type=jnp.float32)
    up = jnp.dot(incoming_activations, fixed_raising_kernel, preferred_element_type=jnp.float32)
    inner_neurons = (jax.nn.silu(gate) * up).astype(jnp.bfloat16)
    order_quantity = jnp.dot(inner_neurons, correction_narrower.T, preferred_element_type=jnp.float32).astype(jnp.bfloat16)
    reverse_quantity = jnp.dot(objective_cotangents, correction_widener.T, preferred_element_type=jnp.float32).astype(jnp.bfloat16)
    earlier_example = jnp.dot(reverse_quantity.T, inner_neurons, preferred_element_type=jnp.float32)
    later_example = jnp.dot(order_quantity.T, objective_cotangents, preferred_element_type=jnp.float32)
    return (earlier_example, later_example)

def reference(incoming_activations, objective_cotangents, fixed_gating_kernel, fixed_raising_kernel, correction_narrower, correction_widener, cutoff_limits):
    earlier_example, later_example = lax.map(lambda example_matching: example_contributions(example_matching, fixed_gating_kernel, fixed_raising_kernel, correction_narrower, correction_widener), (incoming_activations, objective_cotangents))
    norm_a = jnp.sqrt(lax.optimization_barrier(jnp.sum(earlier_example * earlier_example, axis=(1, 2))))
    norm_b = jnp.sqrt(lax.optimization_barrier(jnp.sum(later_example * later_example, axis=(1, 2))))
    factor_a = cutoff_limits[0] / (norm_a + 0.01)
    factor_b = cutoff_limits[1] / (norm_b + 0.01)
    grad_a = lax.optimization_barrier(jnp.sum(factor_a[:, None, None] * earlier_example, axis=0))
    grad_b = lax.optimization_barrier(jnp.sum(factor_b[:, None, None] * later_example, axis=0))
    return (grad_a, grad_b)
```

```python
import functools

import jax
import jax.numpy as jnp
from jax import lax
from jax.experimental import pallas as pl
from jax.experimental.pallas import tpu as pltpu
from jax.sharding import Mesh
from jax.sharding import PartitionSpec as P


F32, BF16 = jnp.float32, jnp.bfloat16
WIDTHS = (256, 256, 256, 128)
TILE = 256
ZRING = ("dp", "tensor_0")
COLUMN = ("dp", "tensor_0", "tensor_1")


def come_from(v, axis, step):
    n = lax.axis_size(axis)
    return lax.ppermute(v, axis, [((i + step) % n, i) for i in range(n)])


def swap_with(v, axis, mask):
    n = lax.axis_size(axis)
    return lax.ppermute(v, axis, [(i, i ^ mask) for i in range(n)])


def round_the_ring(v, axis):
    half = v.shape[0] // 2
    one, three = come_from(v, axis, 1), come_from(v, axis, -1)
    two = (come_from(one[:half], axis, 1), come_from(three[half:], axis, -1))
    return (v,), (one,), two, (three,)


def gathered(piece, first, second):
    row = jnp.concatenate([p for d in round_the_ring(piece, first) for p in d], axis=0)
    return [p for d in round_the_ring(row, second) for p in d]


def sum_along(v, axis):
    return (v + come_from(v, axis, 1)) + (come_from(v, axis, 2) + come_from(v, axis, 3))


def arrange_kernel(place, *refs):
    pieces, out, sem = refs[:-2], refs[-2], refs[-1]
    z, core, y, x = place[0], place[1], place[2], place[3]
    copies = []
    at = 0
    for far in range(4):
        parts = [(0, 512)] if far != 2 else [(0, 256), (256, 256)]
        there = lax.rem(z + far, 4)
        doc, low = there // 2, lax.rem(there, 2)
        for flip in range(2):
            shard = 2 * low + (core if flip == 0 else 1 - core)
            row = lax.rem(shard - y + 4, 4)
            for start, size in parts:
                for block in range(4):
                    col = row * 4 + lax.rem(block - x + 4, 4)
                    copies.append(
                        pltpu.make_async_copy(
                            pieces[at].at[:, pl.ds(block * 256, 256)],
                            out.at[
                                pl.ds(pl.multiple_of(doc * 512 + start, 256), size),
                                pl.ds(pl.multiple_of(col * 256, 256), 256),
                            ],
                            sem.at[len(copies)],
                        )
                    )
                at += 1
    for c in copies:
        c.start()
    for c in copies:
        c.wait()


def arrange(place, pieces):
    return pl.pallas_call(
        arrange_kernel,
        out_shape=jax.ShapeDtypeStruct((1024, 4096), BF16),
        in_specs=[pl.BlockSpec(memory_space=pltpu.SMEM)] + [pl.BlockSpec(memory_space=pl.ANY)] * len(pieces),
        out_specs=pl.BlockSpec(memory_space=pltpu.VMEM),
        scratch_shapes=[pltpu.SemaphoreType.DMA((40,))],
        compiler_params=pltpu.CompilerParams(vmem_limit_bytes=20 * 2**20),
        cost_estimate=pl.CostEstimate(flops=4_000_000_000, bytes_accessed=2 * 2**23, transcendentals=0),
        name="arrange",
    )(place, *pieces)


def block_kernel(x_ref, g0, g1, g2a, g2b, g3, u0, u1, u2a, u2b, u3, a_ref, back_ref, low_ref, grad_ref):
    def dot(a, b):
        return jnp.dot(a, b, preferred_element_type=F32)

    x = x_ref[...]
    gate = dot(x[:, 0:1024], g0[...])
    gate += dot(x[:, 1024:2048], g1[...])
    gate += dot(x[:, 2048:2560], g2a[...])
    gate += dot(x[:, 2560:3072], g2b[...])
    gate += dot(x[:, 3072:4096], g3[...])

    def cols(dx, dys):
        return jnp.concatenate([x[:, (dy * 4 + dx) * 256 : (dy * 4 + dx + 1) * 256] for dy in dys], axis=1)

    up = dot(cols(0, (0, 1, 2, 3)), u0[...])
    up += dot(cols(1, (0, 1, 2, 3)), u1[...])
    up += dot(cols(2, (0, 1)), u2a[...])
    up += dot(cols(2, (2, 3)), u2b[...])
    up += dot(cols(3, (0, 1, 2, 3)), u3[...])
    hidden = ((gate / (1.0 + jnp.exp(-gate))) * up).astype(BF16)
    low_ref[...] = lax.dot_general(a_ref[...], hidden, (((1,), (1,)), ((), ())), preferred_element_type=F32)
    term = dot(back_ref[...], hidden)[None]
    m = pl.program_id(0)

    @pl.when(lax.rem(m, 2) == 0)
    def _():
        grad_ref[...] = term

    @pl.when(lax.rem(m, 2) == 1)
    def _():
        grad_ref[...] += term


def block(x, gates, ups, a, back):
    width = a.shape[1]
    whole = lambda v: pl.BlockSpec(v.shape, lambda m: (0, 0))
    return pl.pallas_call(
        block_kernel,
        grid=(1024 // TILE,),
        out_shape=(
            jax.ShapeDtypeStruct((16, 1024), F32),
            jax.ShapeDtypeStruct((2, 16, width), F32),
        ),
        in_specs=[pl.BlockSpec((TILE, 4096), lambda m: (m, 0))]
        + [whole(v) for v in (*gates, *ups, a)]
        + [pl.BlockSpec((16, TILE), lambda m: (0, m))],
        out_specs=(
            pl.BlockSpec((16, TILE), lambda m: (0, m)),
            pl.BlockSpec((1, 16, width), lambda m: (m // 2, 0, 0)),
        ),
        compiler_params=pltpu.CompilerParams(
            dimension_semantics=("arbitrary",), vmem_limit_bytes=32 * 2**20
        ),
        cost_estimate=pl.CostEstimate(
            flops=4 * 1024 * 4096 * width, bytes_accessed=2**23 + 4096 * width * 4, transcendentals=1024 * width
        ),
        name="block",
    )(x, *gates, *ups, a, back)


def body(
    incoming_activations,
    objective_cotangents,
    fixed_gating_kernel,
    fixed_raising_kernel,
    correction_narrower,
    correction_widener,
    cutoff_limits,
):
    doc = lax.axis_index("dp")
    first = doc == 0
    half = correction_narrower.shape[1] // 2
    starts = [sum(WIDTHS[:k]) for k in range(len(WIDTHS))]

    def mine(v, start, width):
        return jnp.where(first, v[:, start : start + width], v[:, half + start : half + start + width])

    def by_doc(own, other, axis):
        return jnp.concatenate([jnp.where(first, own, other), jnp.where(first, other, own)], axis=axis)

    gates, ups = [], []
    for start, width in zip(starts, WIDTHS):
        gates.append(gathered(mine(fixed_gating_kernel, start, width), "x", "y"))
        ups.append(gathered(mine(fixed_raising_kernel, start, width), "y", "x"))

    pieces = []
    for parts in round_the_ring(incoming_activations[0], ZRING):
        pieces.extend(parts)
        pieces.extend(swap_with(p, "tensor_1", 1) for p in parts)
    z = 2 * doc + lax.axis_index("tensor_0")
    place = jnp.stack([z, lax.axis_index("tensor_1"), lax.axis_index("y"), lax.axis_index("x")]).astype(jnp.int32)
    x = arrange(place, pieces)

    cot = objective_cotangents[0]
    back = lax.dot_general(correction_widener, cot, (((1,), (1,)), ((), ())), preferred_element_type=F32)
    back = back + swap_with(back, "tensor_1", 1)
    back = (back + swap_with(back, "tensor_0", 1)).astype(BF16)
    back = by_doc(back, swap_with(back, "dp", 1), 1)

    low, grads = None, []
    for k, (start, width) in enumerate(zip(starts, WIDTHS)):
        part, grad = block(x, gates[k], ups[k], mine(correction_narrower, start, width), back)
        low = part if low is None else low + part
        grad = jnp.concatenate([grad[0], grad[1]], axis=1)
        if k < len(WIDTHS) - 1:
            grad = sum_along(sum_along(grad, "x"), "y")
        grads.append(grad)

    own_low = jnp.where(first, low[:, :512], low[:, 512:])
    other_low = jnp.where(first, low[:, 512:], low[:, :512])
    total = own_low
    for mask in range(1, 8):
        total = total + swap_with(other_low if mask & 4 else own_low, COLUMN, mask)
    grad_b = jnp.dot(total.astype(BF16), cot, preferred_element_type=F32)

    both = jnp.concatenate([grad_b, grads[-1]], axis=1)
    both = sum_along(sum_along(both, "x"), "y")
    grad_b = both[:, :1024]
    grads[-1] = both[:, 1024:]

    squares = []
    for d in range(2):
        squares.append(sum(jnp.sum(jnp.square(g[:, d * w : (d + 1) * w])) for g, w in zip(grads, WIDTHS)))
    square_b = jnp.sum(jnp.square(grad_b))
    squares.append(jnp.where(first, square_b, 0.0))
    squares.append(jnp.where(first, 0.0, square_b))
    squares = jnp.broadcast_to(jnp.stack(squares)[:, None], (4, 128))
    squares = jnp.concatenate([squares, squares], axis=0)
    total = squares
    for mask in range(1, 8):
        total = total + swap_with(squares, COLUMN, mask)
    norms = jnp.sqrt(total[:4, 0]) + 0.01
    factor_a = cutoff_limits[0] / norms[:2]
    factor_b = cutoff_limits[1] / norms[2:]

    other_b = swap_with(grad_b, "dp", 1)
    out_b = jnp.where(first, factor_b[0], factor_b[1]) * grad_b + jnp.where(first, factor_b[1], factor_b[0]) * other_b
    lower, upper = [], []
    for g, w in zip(grads, WIDTHS):
        other = swap_with(g, "dp", 1)
        lo, hi = jnp.where(first, g, other), jnp.where(first, other, g)
        lower.append(factor_a[0] * lo[:, :w] + factor_a[1] * lo[:, w:])
        upper.append(factor_a[0] * hi[:, :w] + factor_a[1] * hi[:, w:])
    return (jnp.concatenate(lower + upper, axis=1), out_b)


def solution(mesh):
    split = Mesh(
        mesh.devices.reshape(mesh.shape["dp"], 4, 4, 2, 2),
        ("dp", "y", "x", "tensor_0", "tensor_1"),
    )
    tensor, seq = ("tensor_0", "tensor_1"), ("y", "x")
    placed = (
        P("dp", seq, tensor),
        P("dp", seq, tensor),
        P(seq, tensor),
        P(seq, tensor),
        P(None, tensor),
        P(None, tensor),
        P(),
    )
    return jax.shard_map(
        body,
        mesh=split,
        in_specs=placed,
        out_specs=(P(None, tensor), P(None, tensor)),
        check_vma=False,
    )
```

```python
import jax
import jax.numpy as jnp
from jax import lax
from jax.experimental import pallas as pl
from jax.experimental.pallas import tpu as pltpu
from jax.sharding import Mesh
from jax.sharding import PartitionSpec as P


F32, BF16 = jnp.float32, jnp.bfloat16
WIDTHS = (512, 384)
TILE = 256
ZRING = ("dp", "tensor_0")


def swap(v, axis, mask):
    n = lax.axis_size(axis)
    return lax.ppermute(v, axis, [(i, i ^ mask) for i in range(n)])


def round_the_ring(v, axis):
    half = v.shape[0] // 2
    one, three = swap(v, axis, 1), swap(v, axis, 3)
    top, bottom = three[:half], one[half:]
    return [v, one, swap(top, axis, 1), swap(bottom, axis, 3), three]


def sum_along(v, axis):
    return (v + swap(v, axis, 1)) + (swap(v, axis, 2) + swap(v, axis, 3))


def move(copies):
    for c in copies:
        c.start()
    for c in copies:
        c.wait()


def rows_kernel(*refs):
    pieces, outs, sem = refs[:10], refs[10:-1], refs[-1]
    copies = []
    for kind in range(2):
        at = 0
        for p in pieces[kind * 5 : kind * 5 + 5]:
            start = 0
            for k, width in enumerate(WIDTHS):
                copies.append(
                    pltpu.make_async_copy(
                        p.at[:, pl.ds(start, width)],
                        outs[kind * len(WIDTHS) + k].at[pl.ds(at, p.shape[0]), :],
                        sem.at[len(copies)],
                    )
                )
                start += width
            at += p.shape[0]
    move(copies)


def rows(gate_pieces, up_pieces):
    any_ = pl.BlockSpec(memory_space=pl.ANY)
    outs = pl.pallas_call(
        rows_kernel,
        out_shape=tuple(jax.ShapeDtypeStruct((1024, w), BF16) for w in WIDTHS * 2),
        in_specs=[any_] * 10,
        out_specs=(pl.BlockSpec(memory_space=pltpu.VMEM),) * (2 * len(WIDTHS)),
        scratch_shapes=[pltpu.SemaphoreType.DMA((10 * len(WIDTHS),))],
        compiler_params=pltpu.CompilerParams(vmem_limit_bytes=12 * 2**20),
        cost_estimate=pl.CostEstimate(flops=3_000_000_000, bytes_accessed=2 * 3670016, transcendentals=0),
        name="rows",
    )(*gate_pieces, *up_pieces)
    return outs[: len(WIDTHS)], outs[len(WIDTHS) :]


def arrange_kernel(place, *refs):
    pieces, out, sem = refs[:-2], refs[-2], refs[-1]
    z, core, y, x = place[0], place[1], place[2], place[3]
    copies = []
    for mask in range(4):
        there = z ^ mask
        doc, low = there // 2, lax.rem(there, 2)
        for flip in range(2):
            row = (2 * low + (core ^ flip)) ^ y
            for block in range(4):
                col = row * 4 + (x ^ block)
                copies.append(
                    pltpu.make_async_copy(
                        pieces[2 * mask + flip].at[:, pl.ds(block * 256, 256)],
                        out.at[
                            pl.ds(pl.multiple_of(doc * 512, 512), 512),
                            pl.ds(pl.multiple_of(col * 256, 256), 256),
                        ],
                        sem.at[len(copies)],
                    )
                )
    move(copies)


def arrange(place, pieces):
    return pl.pallas_call(
        arrange_kernel,
        out_shape=jax.ShapeDtypeStruct((1024, 4096), BF16),
        in_specs=[pl.BlockSpec(memory_space=pltpu.SMEM)] + [pl.BlockSpec(memory_space=pl.ANY)] * 8,
        out_specs=pl.BlockSpec(memory_space=pltpu.VMEM),
        scratch_shapes=[pltpu.SemaphoreType.DMA((32,))],
        compiler_params=pltpu.CompilerParams(vmem_limit_bytes=12 * 2**20),
        cost_estimate=pl.CostEstimate(flops=4_000_000_000, bytes_accessed=2 * 2**23, transcendentals=0),
        name="arrange",
    )(place, *pieces)


def block_kernel(x_ref, *refs):
    gates, ups = refs[:5], refs[5:10]
    a_ref, back_ref, low_ref, grad_ref, both, hidden = refs[10:]
    n = pl.program_id(0)

    at = 0
    for g in gates:
        both[pl.ds(at, g.shape[0]), :128] = g[...]
        at += g.shape[0]
    at = 0
    for u in ups:
        for k in range(u.shape[0] // 256):
            row = (at // 256 % 4) * 4 + at // 1024
            both[pl.ds(row * 256, 256), 128:] = u[pl.ds(k * 256, 256), :]
            at += 256
    for m in range(1024 // TILE):
        tokens = slice(m * TILE, (m + 1) * TILE)
        sums = jnp.dot(x_ref[tokens, :], both[...], preferred_element_type=F32)
        gate, up = sums[:, :128], sums[:, 128:]
        hidden[tokens, :] = ((gate / (1.0 + jnp.exp(-gate))) * up).astype(BF16)
    low = lax.dot_general(a_ref[...], hidden[...], (((1,), (1,)), ((), ())), preferred_element_type=F32)
    low_ref[...] = jnp.where(n == 0, 0.0, low_ref[...]) + low
    for d in range(2):
        tokens = slice(d * 512, (d + 1) * 512)
        grad_ref[d] = jnp.dot(back_ref[:, tokens], hidden[tokens, :], preferred_element_type=F32)


def block(x, gates, ups, a, back):
    width = a.shape[1]
    tile = lambda v: pl.BlockSpec((v.shape[0], 128), lambda n: (0, n))
    whole = pl.BlockSpec(memory_space=pltpu.VMEM)
    return pl.pallas_call(
        block_kernel,
        grid=(width // 128,),
        out_shape=(
            jax.ShapeDtypeStruct((16, 1024), F32),
            jax.ShapeDtypeStruct((2, 16, width), F32),
        ),
        in_specs=[whole] + [tile(v) for v in (*gates, *ups, a)] + [whole],
        out_specs=(
            pl.BlockSpec((16, 1024), lambda n: (0, 0)),
            pl.BlockSpec((2, 16, 128), lambda n: (0, 0, n)),
        ),
        scratch_shapes=[pltpu.VMEM((4096, 256), BF16), pltpu.VMEM((1024, 128), BF16)],
        compiler_params=pltpu.CompilerParams(dimension_semantics=("arbitrary",), vmem_limit_bytes=28 * 2**20),
        cost_estimate=pl.CostEstimate(
            flops=4 * 1024 * 4096 * width, bytes_accessed=4096 * width * 4, transcendentals=1024 * width
        ),
        name="block",
    )(x, *gates, *ups, a, back)


def compute(
    incoming_activations,
    objective_cotangents,
    fixed_gating_kernel,
    fixed_raising_kernel,
    correction_narrower,
    correction_widener,
    cutoff_limits,
):
    doc = lax.axis_index("dp")
    first = doc == 0
    half = correction_narrower.shape[1] // 2
    starts = [sum(WIDTHS[:k]) for k in range(len(WIDTHS))]

    def mine(v, start, width):
        return jnp.where(first, v[:, start : start + width], v[:, half + start : half + start + width])

    inner = sum(WIDTHS)
    gate_rows, up_rows = rows(
        round_the_ring(mine(fixed_gating_kernel, 0, inner), "x"),
        round_the_ring(mine(fixed_raising_kernel, 0, inner), "y"),
    )
    gates = [round_the_ring(r, "y") for r in gate_rows]
    ups = [round_the_ring(r, "x") for r in up_rows]

    pieces = []
    for mask in range(4):
        p = incoming_activations[0] if mask == 0 else swap(incoming_activations[0], ZRING, mask)
        pieces += [p, swap(p, "tensor_1", 1)]
    z = 2 * doc + lax.axis_index("tensor_0")
    place = jnp.stack([z, lax.axis_index("tensor_1"), lax.axis_index("y"), lax.axis_index("x")]).astype(jnp.int32)
    x = arrange(place, pieces)

    cot = objective_cotangents[0]
    back = lax.dot_general(correction_widener, cot, (((1,), (1,)), ((), ())), preferred_element_type=F32)
    back = back + swap(back, "tensor_1", 1)
    back = (back + swap(back, "tensor_0", 1)).astype(BF16)
    other_back = swap(back, "dp", 1)
    back = jnp.concatenate([jnp.where(first, back, other_back), jnp.where(first, other_back, back)], axis=1)

    low, grads = None, []
    for k, (start, width) in enumerate(zip(starts, WIDTHS)):
        part, grad = block(x, gates[k], ups[k], mine(correction_narrower, start, width), back)
        low = part if low is None else low + part
        grad = jnp.concatenate([grad[0], grad[1]], axis=1)
        if k < len(WIDTHS) - 1:
            grad = sum_along(sum_along(grad, "x"), "y")
        grads.append(grad)

    low = low + swap(low, "tensor_1", 1)
    own_low = jnp.where(first, low[:, :512], low[:, 512:])
    other_low = jnp.where(first, low[:, 512:], low[:, :512])
    low = (own_low + swap(own_low, ZRING, 1)) + (swap(other_low, ZRING, 2) + swap(other_low, ZRING, 3))
    grad_b = jnp.dot(low.astype(BF16), cot, preferred_element_type=F32)

    both = jnp.concatenate([grad_b, grads[-1]], axis=1)
    both = sum_along(sum_along(both, "x"), "y")
    others = [swap(g, "dp", 1) for g in (*grads[:-1], both)]

    squares = norm_squares(grads[:-1], both, doc)
    squares = squares + swap(squares, "tensor_1", 1)
    squares = (squares + swap(squares, ZRING, 1)) + (swap(squares, ZRING, 2) + swap(squares, ZRING, 3))
    return finish(squares, cutoff_limits, doc, grads[:-1], both, others)


def squares_kernel(doc, *refs):
    early, both, out = refs[:-2], refs[-2], refs[-1]
    last = WIDTHS[-1]

    def total(v):
        return jnp.sum(jnp.sum(v * v, axis=1, keepdims=True), axis=0, keepdims=True)

    sums = []
    for d in range(2):
        s = total(both[:, 1024 + d * last : 1024 + (d + 1) * last])
        for g, w in zip(early, WIDTHS):
            s += total(g[:, d * w : (d + 1) * w])
        sums.append(s)
    b = total(both[:, :1024])
    sums.append(jnp.where(doc[0] == 0, b, 0.0))
    sums.append(jnp.where(doc[0] == 0, 0.0, b))
    row = lax.broadcasted_iota(jnp.int32, (8, 128), 0)
    value = jnp.zeros((8, 128), F32)
    for k, s in enumerate(sums):
        value = jnp.where(row == k, s, value)
    out[...] = value


def norm_squares(early, both, doc):
    smem, vmem = pl.BlockSpec(memory_space=pltpu.SMEM), pl.BlockSpec(memory_space=pltpu.VMEM)
    return pl.pallas_call(
        squares_kernel,
        out_shape=jax.ShapeDtypeStruct((8, 128), F32),
        in_specs=[smem] + [vmem] * (len(early) + 1),
        out_specs=vmem,
        compiler_params=pltpu.CompilerParams(vmem_limit_bytes=8 * 2**20),
        name="norm_squares",
    )(doc.reshape(1).astype(jnp.int32), *early, both)


def finish_kernel(squares, limits, doc, *refs):
    n = len(WIDTHS)
    own, other, out_a, out_b = refs[:n], refs[n : 2 * n], refs[-2], refs[-1]
    norms = jnp.sqrt(squares[...]) + 0.01
    limit = jnp.where(lax.broadcasted_iota(jnp.int32, (8, 128), 0) < 2, limits[0], limits[1])
    factors = limit / norms
    fa0, fa1, fb0, fb1 = (factors[k : k + 1, :1] for k in range(4))
    first = doc[0] == 0
    out_b[...] = jnp.where(first, fb0, fb1) * own[-1][:, :1024] + jnp.where(first, fb1, fb0) * other[-1][:, :1024]
    half = sum(WIDTHS)
    at = 0
    for k, w in enumerate(WIDTHS):
        base = 1024 if k == n - 1 else 0
        mine = fa0 * own[k][:, base : base + w] + fa1 * own[k][:, base + w : base + 2 * w]
        theirs = fa0 * other[k][:, base : base + w] + fa1 * other[k][:, base + w : base + 2 * w]
        out_a[:, at : at + w] = jnp.where(first, mine, theirs)
        out_a[:, half + at : half + at + w] = jnp.where(first, theirs, mine)
        at += w


def finish(squares, limits, doc, early, both, others):
    smem, vmem = pl.BlockSpec(memory_space=pltpu.SMEM), pl.BlockSpec(memory_space=pltpu.VMEM)
    return pl.pallas_call(
        finish_kernel,
        out_shape=(
            jax.ShapeDtypeStruct((16, 2 * sum(WIDTHS)), F32),
            jax.ShapeDtypeStruct((16, 1024), F32),
        ),
        in_specs=[vmem, smem, smem] + [vmem] * (2 * len(WIDTHS)),
        out_specs=(vmem, vmem),
        compiler_params=pltpu.CompilerParams(vmem_limit_bytes=8 * 2**20),
        name="finish",
    )(squares, limits, doc.reshape(1).astype(jnp.int32), *early, both, *others)


def solution(mesh):
    split = Mesh(
        mesh.devices.reshape(mesh.shape["dp"], 4, 4, 2, 2),
        ("dp", "y", "x", "tensor_0", "tensor_1"),
    )
    tensor, seq = ("tensor_0", "tensor_1"), ("y", "x")
    placed = (
        P("dp", seq, tensor),
        P("dp", seq, tensor),
        P(seq, tensor),
        P(seq, tensor),
        P(None, tensor),
        P(None, tensor),
        P(),
    )
    return jax.shard_map(
        compute,
        mesh=split,
        in_specs=placed,
        out_specs=(P(None, tensor), P(None, tensor)),
        check_vma=False,
    )
```
